32 devices in a mesh: wide: 16 (over z, x, core), narrow: 2 (over y).
Axes of the slice: x: 2, y: 2, z: 4, core: 2. Of those that a mesh axis runs over, the one named last changes fastest.
Arguments:
- tokens: bfloat16 [2, 32768, 768], P(None, ('wide', 'narrow')), may hold values from -6 to 6
- grad_out: bfloat16 [2, 32768, 768], P(None, ('wide', 'narrow')), may hold values from -6 to 6
- route_ids: int32 [2, 32768], P(None, ('wide', 'narrow')), may hold values from 0 to 15, as said below
- slot_ids: int32 [2, 32768], P(None, ('wide', 'narrow')), may hold values from 0 to 63, as said below
- keep_ids: int32 [2, 32768], P(None, ('wide', 'narrow')), may hold values from 0 to 1, as said below
- gain_one: float32 [768], replicated, may hold values from 0.5 to 1.5
- w_query: bfloat16 [768, 768], replicated, may hold values from -0.21875 to 0.21875
- w_key: bfloat16 [768, 768], replicated, may hold values from -0.21875 to 0.21875
- w_value: bfloat16 [768, 768], replicated, may hold values from -0.21875 to 0.21875
- w_out: bfloat16 [768, 768], replicated, may hold values from -4 to 4
- gain_two: float32 [768], replicated, may hold values from 0.5 to 1.5
- w_route: bfloat16 [768, 16], replicated, may hold values from -0.21875 to 0.21875
- embed: float32 [16, 16], replicated, may hold values from -6 to 6
- w_in: bfloat16 [16, 768, 3072], P('wide', None, 'narrow'), may hold values from -0.21875 to 0.21875
- w_outer: bfloat16 [16, 3072, 768], P('wide', 'narrow'), may hold values from -1.75 to 1.75
Outputs:
- block_out: bfloat16 [2, 32768, 768], P(None, ('wide', 'narrow'))
- grad_tokens: bfloat16 [2, 32768, 768], P(None, ('wide', 'narrow'))
- grad_gain_one: float32 [768], replicated
- grad_w_query: float32 [768, 768], replicated
- grad_w_key: float32 [768, 768], replicated
- grad_w_value: float32 [768, 768], replicated
- grad_w_out: float32 [768, 768], replicated
- grad_gain_two: float32 [768], replicated
- grad_w_route: float32 [768, 16], replicated
- grad_embed: float32 [16, 16], replicated
- grad_w_in: float32 [16, 768, 3072], P('wide', None, 'narrow')
- grad_w_outer: float32 [16, 3072, 768], P('wide', 'narrow')
The draws below stay inside these ranges and needn't reach their ends.
Inputs may be any that keep to these rules, and one draw needn't show every extreme that they name: `route_ids`: an expert's number for every token. `slot_ids`: within one aligned block of 1024 tokens of a micro-batch, the kept tokens bound for one expert carry slots 0, 1, 2, ... in token order; a token that would need slot 64 or more is dropped and carries 0. In every block some expert has all 64 slots filled and more tokens than that. `keep_ids`: 1 exactly for the tokens that got a slot; tokens are dropped in token order once an expert's 64 slots of the block are taken.
All inputs are finite; a program needn't handle non-finite values.
Results may differ from the reference program's by a relative error of at most 0.015.
Values may be sent and summed in bfloat16 or wider, within the bound.
A program may use at most 384 MiB of HBM per device.

```python
import jax
import jax.numpy as jnp
from jax import lax

D = 768
HEADS = 12
HEAD_DIM = 64
FF = 3072
RDIM = 16
LENGTH = 1024
MICRO = 2
EXPERTS = 16
TOK_MB = 1024
TOKENS = 32768
CAP = 64


def routing_tables(key):
    base_key, hot_key, order_key = jax.random.split(jax.random.fold_in(key, 11), 3)
    blocks = MICRO * TOKENS // TOK_MB
    base_ids = jax.random.randint(base_key, (blocks, TOK_MB), 0, EXPERTS, dtype=jnp.int32)
    hot_ids = jax.random.randint(hot_key, (blocks, 1), 0, EXPERTS, dtype=jnp.int32)
    orders = jax.vmap(lambda block_key: jax.random.permutation(block_key, TOK_MB))(jax.random.split(order_key, blocks))
    routes = jnp.where(orders <= CAP, hot_ids, base_ids).astype(jnp.int32)
    onehot = (routes[:, :, None] == jnp.arange(EXPERTS, dtype=jnp.int32)[None, None, :]).astype(jnp.int32)
    before = jnp.cumsum(onehot, axis=1) - onehot
    slots = jnp.sum(before * onehot, axis=-1).astype(jnp.int32)
    keeps = (slots < CAP).astype(jnp.int32)
    slots = jnp.where(keeps > 0, slots, 0).astype(jnp.int32)
    return (routes.reshape(MICRO, TOKENS), slots.reshape(MICRO, TOKENS), keeps.reshape(MICRO, TOKENS))


def draw_route_ids(key, part):
    return routing_tables(key)[0]


def draw_slot_ids(key, part):
    return routing_tables(key)[1]


def draw_keep_ids(key, part):
    return routing_tables(key)[2]


def block_levels(rng, extent, cuts, smallest, top_value):
    def one(axis_at, parts):
        draws = jax.random.uniform(jax.random.fold_in(jax.random.fold_in(rng, 6), axis_at), (parts,), jnp.float32, smallest / len(cuts), top_value / len(cuts))
        return jnp.repeat(jnp.exp(draws), extent[axis_at] // parts).reshape((-1,) + (1,) * (len(extent) - axis_at - 1))

    loudness = one(*cuts[0])
    for cut in cuts[1:]:
        loudness = loudness * one(*cut)
    return loudness


def bell_draw(stream_key, dims, deviation, bound, cuts=(), held_as=jnp.bfloat16):
    loudness = block_levels(stream_key, dims, cuts, -0.22, 0.18) if cuts else 1.0
    array = jax.random.normal(stream_key, dims, jnp.float32) * deviation * loudness
    return jnp.minimum(jnp.maximum(array, -bound), bound).astype(held_as)


def setup_inputs(seed: int = 0) -> dict:
    key_of = jax.random.split(jax.random.key(seed), 16)
    return {
        "tokens": bell_draw(key_of[0], (MICRO, TOKENS, D), 1.0, 6.0, ((1, 32),)),
        "grad_out": bell_draw(key_of[1], (MICRO, TOKENS, D), 1.0, 6.0, ((1, 32),)),
        "route_ids": draw_route_ids(jax.random.fold_in(key_of[15], 71), 0),
        "slot_ids": draw_slot_ids(jax.random.fold_in(key_of[15], 71), 0),
        "keep_ids": draw_keep_ids(jax.random.fold_in(key_of[15], 71), 0),
        "gain_one": jnp.clip(1.0 + 0.1 * jax.random.normal(key_of[5], (D,), jnp.float32), 0.5, 1.5),
        "w_query": bell_draw(key_of[6], (D, D), D ** -0.5, 0.21875),
        "w_key": bell_draw(key_of[7], (D, D), D ** -0.5, 0.21875),
        "w_value": bell_draw(key_of[8], (D, D), D ** -0.5, 0.21875),
        "w_out": bell_draw(key_of[9], (D, D), (max(1, 3 * D // LENGTH)) ** -0.5, 4.0),
        "gain_two": jnp.clip(1.0 + 0.1 * jax.random.normal(key_of[10], (D,), jnp.float32), 0.5, 1.5),
        "w_route": bell_draw(key_of[11], (D, RDIM), D ** -0.5, 0.21875),
        "embed": bell_draw(key_of[12], (EXPERTS, RDIM), 1.0, 6.0, (), jnp.float32),
        "w_in": bell_draw(key_of[13], (EXPERTS, D, FF), D ** -0.5, 0.21875, ((0, 16), (2, 2))),
        "w_outer": bell_draw(key_of[14], (EXPERTS, FF, D), (max(1, FF // (EXPERTS * EXPERTS))) ** -0.5, 1.75, ((0, 16), (1, 2))),
    }


@jax.custom_vjp
def low(v):
    return lax.optimization_barrier(v.astype(jnp.bfloat16)).astype(jnp.float32)

@jax.custom_vjp
def low_back(v):
    return v

def low_keep(v):
    return (low(v), None)

def low_pass(kept, grad):
    return (grad,)

def back_keep(v):
    return (v, None)

def back_low(kept, grad):
    return (low(grad),)
low.defvjp(low_keep, low_pass)
low_back.defvjp(back_keep, back_low)

def layer_norm(values, gain_vec):
    centred = values - lax.optimization_barrier(jnp.mean(values, axis=-1, keepdims=True))
    spread_sq = lax.optimization_barrier(jnp.mean(centred * centred, axis=-1, keepdims=True))
    return centred * lax.rsqrt(spread_sq + 1e-05) * gain_vec

def product(left, right):
    return jnp.dot(left, right, precision=lax.Precision.HIGHEST, preferred_element_type=jnp.float32)

def gate_from(projected, embed_rows, route_row):
    unit_rows = projected * lax.rsqrt(lax.optimization_barrier(jnp.sum(projected * projected, axis=-1, keepdims=True)) + 1.0)
    anchor = embed_rows * lax.rsqrt(lax.optimization_barrier(jnp.sum(embed_rows * embed_rows, axis=-1, keepdims=True)) + 1.0)
    logits = 3.0 * product(unit_rows, anchor.T)
    soft_rows = jax.nn.softmax(logits, axis=-1)
    picked = route_row[:, None] == jnp.arange(soft_rows.shape[1], dtype=jnp.int32)[None, :]
    return lax.optimization_barrier(jnp.sum(jnp.where(picked, soft_rows, 0.0), axis=-1))

def attend_one(queries, keys_in, values_in):
    score_scale = HEAD_DIM ** (-0.5)
    scores = low_back(jnp.einsum('qhd,khd->hqk', queries, keys_in, precision=lax.Precision.HIGHEST) * score_scale)
    soft_rows = low(jax.nn.softmax(scores, axis=-1))
    return jnp.einsum('hqk,khd->qhd', soft_rows, values_in, precision=lax.Precision.HIGHEST)

def expert_one(row_block, first_layer, second_layer):
    pre_act = low_back(product(row_block, first_layer))
    hidden = low(jax.nn.gelu(pre_act, approximate=False))
    return low(low_back(product(hidden, second_layer)))

def forward(params, inputs, route_row, slot_row, keep_row):
    gain_a, wq_full, wk_full, wv_full, wo_full, gain_b, route_weight, embed_rows, first_layers, second_layers = params
    tok_count = inputs.shape[0]
    normed_one = low(layer_norm(inputs, gain_a))
    queries = low(low_back(product(normed_one, wq_full)))
    keys_in = low(low_back(product(normed_one, wk_full)))
    values_in = low(low_back(product(normed_one, wv_full)))
    seq_count = tok_count // LENGTH
    head_shape = (seq_count, LENGTH, HEADS, HEAD_DIM)
    mixed_rows = lax.map(lambda group: jax.checkpoint(attend_one)(*group), (queries.reshape(head_shape), keys_in.reshape(head_shape), values_in.reshape(head_shape)))
    mixed_rows = low(low_back(mixed_rows.reshape(tok_count, D)))
    first_sum = inputs + low_back(product(mixed_rows, wo_full))
    normed_two = low(layer_norm(first_sum, gain_b))
    gate_prob = gate_from(product(normed_two, route_weight), embed_rows, route_row)
    sources = tok_count // TOK_MB
    slot_index = jnp.where(keep_row > 0, route_row * CAP + slot_row, EXPERTS * CAP).astype(jnp.int32)
    slot_index = slot_index.reshape(sources, TOK_MB)

    def scatter_block(block_rows, block_index):
        return jnp.zeros((EXPERTS * CAP, D), jnp.float32).at[block_index].add(block_rows, mode='drop')
    sent_rows = low_back(jax.vmap(scatter_block)(normed_two.reshape(sources, TOK_MB, D), slot_index))
    per_expert = jnp.transpose(sent_rows.reshape(sources, EXPERTS, CAP, D), (1, 0, 2, 3)).reshape(EXPERTS, sources * CAP, D)
    results = lax.map(lambda group: jax.checkpoint(expert_one)(*group), (per_expert, first_layers, second_layers))
    back_rows = jnp.transpose(results.reshape(EXPERTS, sources, CAP, D), (1, 0, 2, 3)).reshape(sources, EXPERTS * CAP, D)

    def take_block(buffer_rows, block_index):
        return jnp.take(buffer_rows, block_index, axis=0, mode='fill', fill_value=0.0)
    returned = jax.vmap(take_block)(back_rows, slot_index).reshape(tok_count, D)
    return first_sum + gate_prob[:, None] * returned

def reference(tokens, grad_out, route_ids, slot_ids, keep_ids, gain_one, w_query, w_key, w_value, w_out, gain_two, w_route, embed, w_in, w_outer):
    params = tuple((item.astype(jnp.float32) for item in (gain_one, w_query, w_key, w_value, w_out, gain_two, w_route, embed, w_in, w_outer)))
    totals = tuple((jnp.zeros(item.shape, jnp.float32) for item in params))
    outputs = []
    input_grads = []
    for micro_step in range(MICRO):

        def forward_one(weights, inputs):
            return forward(weights, inputs, route_ids[micro_step], slot_ids[micro_step], keep_ids[micro_step])
        result_rows, pullback = jax.vjp(forward_one, params, tokens[micro_step].astype(jnp.float32))
        grad_params, grad_inputs = pullback(grad_out[micro_step].astype(jnp.float32))
        totals = tuple((total + part_grad for total, part_grad in zip(totals, grad_params)))
        outputs.append(result_rows.astype(jnp.bfloat16))
        input_grads.append(grad_inputs.astype(jnp.bfloat16))
    return (jnp.stack(outputs), jnp.stack(input_grads), totals[0], totals[1], totals[2], totals[3], totals[4], totals[5], totals[6], totals[7], totals[8], totals[9])
```

```python
import jax
import jax.numpy as jnp
from jax import lax
from jax.experimental import pallas as pl
from jax.experimental.pallas import tpu as pltpu
from jax.sharding import PartitionSpec as P

D = 768
HEADS = 12
HEAD_DIM = 64
LENGTH = 1024
PAIRS = HEADS // 2
F32 = jnp.float32
BF16 = jnp.bfloat16


def nt(left, right, precision=None):
    return lax.dot_general(
        left, right, (((1,), (1,)), ((), ())), precision=precision, preferred_element_type=F32
    )


def tn(left, right):
    return lax.dot_general(left, right, (((0,), (0,)), ((), ())), preferred_element_type=F32)


def attend_forward_kernel(q_ref, k_ref, v_ref, out_ref, stat_ref):
    rows = q_ref.shape[0]
    low_half = lax.broadcasted_iota(jnp.int32, (rows, 128), 1) < HEAD_DIM
    queries = q_ref[...] * jnp.asarray(HEAD_DIM**-0.5, BF16)
    keys = k_ref[...]
    values = v_ref[...]
    zero = jnp.zeros_like(keys)
    one = jnp.ones_like(keys)
    mixed = []
    logs = []
    for half in range(2):
        mine = low_half if half == 0 else jnp.logical_not(low_half)
        scores = nt(queries, jnp.where(mine, keys, zero))
        row_max = jnp.max(scores, axis=-1, keepdims=True)
        weights = jnp.exp(scores - row_max).astype(BF16)
        both = jnp.dot(weights, jnp.where(mine, values, one), preferred_element_type=F32)
        total = pltpu.roll(both, HEAD_DIM, 1)
        mixed.append(both / total)
        logs.append(row_max + jnp.log(both))
    out_ref[...] = jnp.where(low_half, mixed[0], mixed[1]).astype(BF16)
    stats = jnp.where(low_half, logs[1], logs[0]).T
    stat_ref[0:8, :] = stats[HEAD_DIM : HEAD_DIM + 8]
    stat_ref[8:16, :] = stats[0:8]


def attend_forward(qkv_rows):
    count = qkv_rows.shape[0]
    seqs = count // LENGTH
    spec = lambda off: pl.BlockSpec((LENGTH, 128), lambda s, j, off=off: (s, off + j))
    return pl.pallas_call(
        attend_forward_kernel,
        grid=(seqs, PAIRS),
        in_specs=[spec(0), spec(PAIRS), spec(2 * PAIRS)],
        out_specs=[
            spec(0),
            pl.BlockSpec((None, None, 16, LENGTH), lambda s, j: (s, j, 0, 0)),
        ],
        out_shape=[
            jax.ShapeDtypeStruct((count, D), BF16),
            jax.ShapeDtypeStruct((seqs, PAIRS, 16, LENGTH), F32),
        ],
        compiler_params=pltpu.CompilerParams(vmem_limit_bytes=56 << 20),
        cost_estimate=pl.CostEstimate(
            flops=seqs * HEADS * 8 * LENGTH * LENGTH * HEAD_DIM,
            bytes_accessed=count * D * 8,
            transcendentals=seqs * HEADS * LENGTH * LENGTH,
        ),
        name="attend_forward",
    )(qkv_rows, qkv_rows, qkv_rows)


def attend_backward_kernel(q_ref, k_ref, v_ref, o_ref, g_ref, stat_ref, gq_ref, gk_ref, gv_ref):
    rows = q_ref.shape[0]
    scale = HEAD_DIM**-0.5
    low_half = lax.broadcasted_iota(jnp.int32, (rows, 128), 1) < HEAD_DIM
    queries = q_ref[...] * jnp.asarray(scale, BF16)
    keys = k_ref[...]
    values = v_ref[...]
    grads = g_ref[...]
    zero = jnp.zeros_like(keys)
    picker = (
        (lax.broadcasted_iota(jnp.int32, (16, 128), 1) >= HEAD_DIM)
        == (lax.broadcasted_iota(jnp.int32, (16, 128), 0) >= 8)
    ).astype(F32)
    inner = nt(picker, grads.astype(F32) * o_ref[...].astype(F32), lax.Precision.HIGHEST)
    grad_q = []
    grad_k = []
    grad_v = []
    for half in range(2):
        mine = low_half if half == 0 else jnp.logical_not(low_half)
        at = 8 * half
        keys_half = jnp.where(mine, keys, zero)
        weights = jnp.exp(nt(keys_half, queries) - stat_ref[at : at + 1, :])
        grad_soft = nt(jnp.where(mine, values, zero), grads)
        grad_scores = (weights * (grad_soft - inner[at : at + 1, :])).astype(BF16)
        grad_v.append(jnp.dot(weights.astype(BF16), grads, preferred_element_type=F32))
        grad_k.append(jnp.dot(grad_scores, queries, preferred_element_type=F32))
        grad_q.append(tn(grad_scores, keys_half))
    gq_ref[...] = ((grad_q[0] + grad_q[1]) * scale).astype(BF16)
    gk_ref[...] = jnp.where(low_half, grad_k[0], grad_k[1]).astype(BF16)
    gv_ref[...] = jnp.where(low_half, grad_v[0], grad_v[1]).astype(BF16)


def attend_backward(qkv_rows, mixed_rows, grad_mixed, stats):
    count = qkv_rows.shape[0]
    seqs = count // LENGTH
    spec = lambda off: pl.BlockSpec((LENGTH, 128), lambda s, j, off=off: (s, off + j))
    return pl.pallas_call(
        attend_backward_kernel,
        grid=(seqs, PAIRS),
        in_specs=[spec(0), spec(PAIRS), spec(2 * PAIRS), spec(0), spec(0),
            pl.BlockSpec((None, None, 16, LENGTH), lambda s, j: (s, j, 0, 0)),
        ],
        out_specs=[spec(0), spec(0), spec(0)],
        out_shape=[jax.ShapeDtypeStruct((count, D), BF16)] * 3,
        compiler_params=pltpu.CompilerParams(vmem_limit_bytes=56 << 20),
        cost_estimate=pl.CostEstimate(
            flops=seqs * HEADS * 20 * LENGTH * LENGTH * HEAD_DIM,
            bytes_accessed=count * D * 16,
            transcendentals=seqs * HEADS * LENGTH * LENGTH,
        ),
        name="attend_backward",
    )(qkv_rows, qkv_rows, qkv_rows, mixed_rows, grad_mixed, stats)


def layer_norm(values, gain_vec):
    centred = values - jnp.mean(values, axis=-1, keepdims=True)
    spread_sq = jnp.mean(centred * centred, axis=-1, keepdims=True)
    return centred * lax.rsqrt(spread_sq + 1e-05) * gain_vec


def gate_from(projected, embed_rows, route_row):
    unit_rows = projected * lax.rsqrt(jnp.sum(projected * projected, axis=-1, keepdims=True) + 1.0)
    anchor = embed_rows * lax.rsqrt(jnp.sum(embed_rows * embed_rows, axis=-1, keepdims=True) + 1.0)
    logits = 3.0 * jnp.dot(
        unit_rows, anchor.T, precision=lax.Precision.HIGHEST, preferred_element_type=F32
    )
    soft_rows = jax.nn.softmax(logits, axis=-1)
    picked = route_row[:, None] == jnp.arange(soft_rows.shape[1], dtype=jnp.int32)[None, :]
    return jnp.sum(jnp.where(picked, soft_rows, 0.0), axis=-1)


def contract_rows(left, right, precise=None):
    return lax.dot_general(
        left, right, (((0,), (0,)), ((), ())), precision=precise, preferred_element_type=F32
    )


def shifted(value, axis, step):
    count = lax.axis_size(axis)
    return lax.ppermute(value, axis, [(src, (src + step) % count) for src in range(count)])


def exchange(rows):
    return lax.all_to_all(rows, "wide", split_axis=0, concat_axis=0, tiled=True)


def gelu_parts(pre):
    cdf = 0.5 * (1.0 + lax.erf(pre * 0.7071067811865476))
    return pre * cdf, cdf + pre * jnp.exp(-0.5 * pre * pre) * 0.3989422804014327


def expert_pass(rows, grads, parts_in, parts_outer):
    result = 0.0
    grad_rows = 0.0
    terms_in = []
    terms_outer = []
    for first, second in zip(parts_in, parts_outer):
        pre = jnp.dot(rows, first, preferred_element_type=F32)
        hidden, slope = gelu_parts(pre)
        hidden = hidden.astype(BF16)
        result = result + jnp.dot(hidden, second, preferred_element_type=F32)
        grad_pre = (nt(grads, second) * slope).astype(BF16)
        terms_outer.append(contract_rows(hidden, grads))
        terms_in.append(contract_rows(rows, grad_pre))
        grad_rows = grad_rows + nt(grad_pre, first)
    return result.astype(BF16), grad_rows.astype(BF16), terms_in, terms_outer


def local(
    tokens,
    grad_out,
    route_ids,
    slot_ids,
    keep_ids,
    gain_one,
    w_query,
    w_key,
    w_value,
    w_out,
    gain_two,
    w_route,
    embed,
    w_in,
    w_outer,
):
    micro_count, tok_count, width = tokens.shape
    narrow_count = lax.axis_size("narrow")
    expert_count = embed.shape[0]
    slot_cap = max(2, tok_count // expert_count)
    w_qkv = jnp.concatenate([w_query, w_key, w_value], axis=1)
    route_float = w_route.astype(F32)
    slot_columns = jnp.arange(expert_count * slot_cap, dtype=jnp.int32)
    parts_in = [w_in[0]] + [shifted(w_in[0], "narrow", k) for k in range(1, narrow_count)]
    parts_outer = [w_outer[0]] + [shifted(w_outer[0], "narrow", k) for k in range(1, narrow_count)]

    def before(step):
        inputs = tokens[step].astype(F32)
        normed_one, pull_one = jax.vjp(layer_norm, inputs, gain_one)
        normed_low = normed_one.astype(BF16)
        qkv = jnp.dot(normed_low, w_qkv, preferred_element_type=F32).astype(BF16)
        mixed, stats = attend_forward(qkv)
        first_sum = inputs + jnp.dot(mixed, w_out, preferred_element_type=F32)
        normed_two, pull_two = jax.vjp(layer_norm, first_sum, gain_two)
        second_low = normed_two.astype(BF16)
        projected = jnp.dot(second_low, w_route, preferred_element_type=F32)
        gate, pull_gate = jax.vjp(
            lambda proj_in, embed_in: gate_from(proj_in, embed_in, route_ids[step]),
            projected,
            embed,
        )
        slot_index = jnp.where(
            keep_ids[step] > 0, route_ids[step] * slot_cap + slot_ids[step], -1
        )
        table = (slot_index[:, None] == slot_columns[None, :]).astype(BF16)
        grad_sum = grad_out[step].astype(F32)
        sent = contract_rows(table, second_low).astype(BF16)
        arrived = exchange(sent.reshape(expert_count, slot_cap, width)).reshape(-1, width)
        grad_low = (gate[:, None] * grad_sum).astype(BF16)
        grad_buffer = contract_rows(table, grad_low).astype(BF16)
        grad_all = exchange(grad_buffer.reshape(expert_count, slot_cap, width)).reshape(-1, width)
        keep = dict(
            pull_one=pull_one, normed_low=normed_low, qkv=qkv, mixed=mixed, stats=stats,
            first_sum=first_sum, pull_two=pull_two, second_low=second_low, gate=gate,
            pull_gate=pull_gate, table=table, grad_sum=grad_sum,
        )
        return keep, arrived, grad_all

    def home(rows):
        return exchange(rows.reshape(-1, slot_cap, width)).reshape(-1, width)

    def after(kept, back_rows, back_grads):
        returned = jnp.dot(kept["table"], back_rows, preferred_element_type=F32)
        grad_sum = kept["grad_sum"]
        out = (kept["first_sum"] + kept["gate"][:, None] * returned).astype(BF16)
        grad_gate = jnp.sum(grad_sum * returned, axis=-1)
        grad_second = jnp.dot(kept["table"], back_grads, preferred_element_type=F32)
        grad_projected, term_embed = kept["pull_gate"](grad_gate)
        grad_second = grad_second + nt(grad_projected, route_float, lax.Precision.HIGHEST)
        term_route = contract_rows(
            kept["second_low"].astype(F32), grad_projected, lax.Precision.HIGHEST
        )
        grad_first_norm, term_gain_two = kept["pull_two"](grad_second)
        grad_first = grad_sum + grad_first_norm
        grad_branch = grad_first.astype(BF16)
        term_wo = contract_rows(kept["mixed"], grad_branch)
        grad_mixed = nt(grad_branch, w_out).astype(BF16)
        grad_heads = attend_backward(kept["qkv"], kept["mixed"], grad_mixed, kept["stats"])
        terms = [contract_rows(kept["normed_low"], part) for part in grad_heads]
        grad_normed = sum(
            nt(part, weight) for part, weight in zip(grad_heads, (w_query, w_key, w_value))
        )
        grad_input_norm, term_gain_one = kept["pull_one"](grad_normed)
        grad_input = (grad_first + grad_input_norm).astype(BF16)
        return out, grad_input, terms + [term_wo], [term_gain_one, term_gain_two, term_route, term_embed]

    add = lambda left, right: jax.tree.map(jnp.add, left, right)
    everywhere = ("wide", "narrow")
    fronts = [before(step) for step in range(micro_count)]
    terms_in = terms_outer = None
    homes = []
    for kept, arrived, grad_all in fronts:
        result, grad_rows, more_in, more_outer = expert_pass(arrived, grad_all, parts_in, parts_outer)
        homes.append((home(result), home(grad_rows)))
        terms_in = more_in if terms_in is None else add(terms_in, more_in)
        terms_outer = more_outer if terms_outer is None else add(terms_outer, more_outer)
    sum_in, sum_outer = terms_in[0], terms_outer[0]
    for k in range(1, narrow_count):
        sum_in = sum_in + shifted(terms_in[k].astype(BF16), "narrow", -k).astype(F32)
        sum_outer = sum_outer + shifted(terms_outer[k].astype(BF16), "narrow", -k).astype(F32)
    outputs = []
    input_grads = []
    large = small = None
    for (kept, _, _), (back_rows, back_grads) in zip(fronts, homes):
        out, grad_input, more_large, more_small = after(kept, back_rows, back_grads)
        outputs.append(out)
        input_grads.append(grad_input)
        large = more_large if large is None else add(large, more_large)
        small = more_small if small is None else add(small, more_small)
    large = [reduce_large(item) for item in large]
    small = lax.psum(small, everywhere)
    return (
        jnp.stack(outputs),
        jnp.stack(input_grads),
        small[0],
        large[0],
        large[1],
        large[2],
        large[3],
        small[1],
        small[2],
        small[3],
        sum_in[None],
        sum_outer[None],
    )


def reduce_large(item):
    return lax.psum(item.astype(BF16), ("wide", "narrow")).astype(F32)


def solution(mesh):
    placed = (
        P(None, ("wide", "narrow"), None),
        P(None, ("wide", "narrow"), None),
        P(None, ("wide", "narrow")),
        P(None, ("wide", "narrow")),
        P(None, ("wide", "narrow")),
        P(),
        P(),
        P(),
        P(),
        P(),
        P(),
        P(),
        P(),
        P("wide", None, "narrow"),
        P("wide", "narrow", None),
    )
    return jax.shard_map(
        local,
        mesh=mesh,
        in_specs=placed,
        out_specs=(
            P(None, ("wide", "narrow"), None),
            P(None, ("wide", "narrow"), None),
            P(),
            P(),
            P(),
            P(),
            P(),
            P(),
            P(),
            P(),
            P("wide", None, "narrow"),
            P("wide", "narrow", None),
        ),
        check_vma=False,
    )
```
